256 devices in a mesh: blk: 16 (over x, z_hi), slab: 16 (over z_lo, y, core).
Axes of the slice: x: 4, y: 4, z: 8 (z_hi: 4, z_lo: 2; z = z_hi * 2 + z_lo), core: 2. Of those that a mesh axis runs over, the one named last changes fastest.
Arguments:
- zeta_sets: bfloat16 [16, 16384, 2048], P('blk', 'slab'), may hold values from -6 to 6
- coef_blocks: bfloat16 [64, 2, 2048, 256], P('blk', None, 'slab'), may hold values from -0.09375 to 0.09375
- pair_table: int32 [64, 2], P('blk'), may hold values from 0 to 1, each once within a row
- band_counts: int32 [64], P('blk'), may hold values from 64 to 256
- orbitals: bfloat16 [64, 16384, 256], P('blk', 'slab'), may hold values from -0.046875 to 0.046875
Outputs:
- exchange_field: float32 [64, 16384, 256], P('blk', 'slab')
- intersection: float32 [64, 256, 256], P('blk')
The draws below stay inside these ranges and needn't reach their ends.
Inputs may be any that keep to these rules, and one draw needn't show every extreme that they name: Each row of pair_table names every number from 0 to 1 once.
All inputs are finite; a program needn't handle non-finite values.
Results may differ from the reference program's by a relative error of at most 0.0003.
Values may be sent and summed in bfloat16 or wider, within the bound.
A program may use at most 64 MiB of HBM per device.

```python
import jax
import jax.numpy as jnp
from jax import lax

N_MU = 2048
BMAX = 256
SETS_GRP = 1
K_GRP = 4
WIN = 2
NSETS = 16
KPTS = 64
NCELLS = 16384
N_BLK = 16


def place_ends(entries, key, low, largest):
    longest = entries.shape.index(max(entries.shape))
    spots = []
    for shift in (0, 1):
        where = [jax.random.randint(jax.random.fold_in(key, axis), (), 0, length) for axis, length in enumerate(entries.shape)]
        where[longest] = (where[longest] + shift) % entries.shape[longest]
        spots.append(tuple(where))
    return entries.at[spots[0]].set(low).at[spots[1]].set(largest)


def shard_levels(own_key, dims, shards, low, high):
    level = 1.0
    for axis_at, parts in shards:
        draws = jax.random.uniform(jax.random.fold_in(jax.random.fold_in(own_key, 6), axis_at), (parts,), jnp.float32, low / len(shards), high / len(shards))
        level = level * jnp.repeat(jnp.exp(draws), dims[axis_at] // parts).reshape((-1,) + (1,) * (len(dims) - 1 - axis_at))
    return level


def scatter_about(own_key, extent, spread, limit, cuts=(), kind=jnp.bfloat16):
    result = spread * jax.random.normal(own_key, extent, jnp.float32)
    if cuts:
        result = result * shard_levels(own_key, extent, cuts, -0.22, 0.18)
    return jnp.clip(result, -limit, limit).astype(kind)


def setup_inputs(seed: int = 0) -> dict:
    key_list = jax.random.split(jax.random.key(seed), 6)
    return {
        "zeta_sets": scatter_about(key_list[0], (NSETS, NCELLS, N_MU), 1.0, 6.0, ((0, 16), (1, 16))),
        "coef_blocks": scatter_about(key_list[1], (KPTS, WIN, N_MU, BMAX), (WIN * N_MU) ** -0.5, 0.09375, ((0, 16), (2, 16))),
        "pair_table": jax.vmap(lambda own: jax.random.permutation(own, WIN))(jax.random.split(key_list[2], KPTS)).reshape((KPTS, WIN)).astype(jnp.int32),
        "band_counts": place_ends(jax.random.randint(key_list[3], (KPTS,), BMAX // 4, BMAX + 1), jax.random.fold_in(key_list[3], 1), BMAX // 4, BMAX).astype(jnp.int32),
        "orbitals": scatter_about(key_list[4], (KPTS, NCELLS, BMAX), NCELLS ** -0.5, 0.046875, ((0, 16), (1, 16))),
    }


def reference(zeta_sets, coef_blocks, pair_table, band_counts, orbitals):
    inverse = jnp.argsort(pair_table, axis=1).astype(jnp.int32)
    ordered = jnp.take_along_axis(coef_blocks, inverse[:, :, None, None], axis=1)
    keep = jnp.arange(BMAX, dtype=jnp.int32)[None, :] < band_counts[:, None]

    def one_kpoint(kpoint):
        group = kpoint // K_GRP
        coef_row = lax.dynamic_index_in_dim(ordered, kpoint, 0, keepdims=False)

        def add_set(window, total):
            source = (group - window // SETS_GRP + N_BLK) % N_BLK
            first = (source * SETS_GRP + window % SETS_GRP).astype(jnp.int32)
            zeta_slab = lax.dynamic_index_in_dim(zeta_sets, first, 0, keepdims=False).astype(jnp.float32)
            block = lax.dynamic_index_in_dim(coef_row, window, 0, keepdims=False).astype(jnp.float32)
            return total + jnp.dot(zeta_slab, block, preferred_element_type=jnp.float32)

        return lax.fori_loop(0, WIN, add_set, jnp.zeros((NCELLS, BMAX), jnp.float32))

    fields = lax.map(one_kpoint, jnp.arange(KPTS, dtype=jnp.int32))
    exchange_field = jnp.where(keep[:, None, :], fields, jnp.zeros((), jnp.float32))
    masked = jnp.where(keep[:, None, :], orbitals.astype(jnp.float32), jnp.zeros((), jnp.float32))
    intersection = jnp.einsum("kca,kcb->kab", masked, exchange_field, precision=lax.Precision.HIGHEST)
    return exchange_field, intersection
```

```python
import functools

import jax
import jax.numpy as jnp
from jax import lax
from jax.experimental import pallas as pl
from jax.experimental.pallas import tpu as pltpu
from jax.sharding import PartitionSpec as P

NZ, NY, NC = 2, 4, 2
LEVELS = 32767.0
TILE = 256


def slab_at(z, y, c):
    return (z * NY + y) * NC + c


def kernel(
    zeta_in, coef_in, orb_in, field_out, inter_out,
    zeta, coef, orb, psend, precv, ssend, srecv, field,
    part, rsib, half, ry, quarter, rz, final,
    load_sem, pair_sem, pair_out, cz_sem, ag_sem, ag_out, p_sem, p_out, ar_sem, ar_out, store_sem,
):
    kpts = orb.shape[0]
    rows = zeta.shape[0]
    tile = min(TILE, rows)
    tiles = rows // tile
    blk, slab = lax.axis_index("blk"), lax.axis_index("slab")
    nblk = lax.axis_size("blk")
    c = lax.rem(slab, NC)
    y = lax.rem(slab // NC, NY)
    z = slab // (NC * NY)
    after, before = lax.rem(blk + 1, nblk), lax.rem(blk + nblk - 1, nblk)
    ys = [lax.rem(y + d, NY) for d in range(NY)]
    at_y = [{"slab": slab_at(z, ys[d], c)} for d in range(NY)]
    at_z = {"slab": slab_at(1 - z, y, c)}
    at_c = {"slab": slab_at(z, y, 1 - c)}
    at_after = {"blk": after, "slab": slab}

    def near(other, zz):
        return {"blk": other, "slab": slab_at(zz, y, c)}

    def send(src, dst, out, arrived, where):
        copy = pltpu.make_async_remote_copy(
            src_ref=src, dst_ref=dst, send_sem=out, recv_sem=arrived,
            device_id=where, device_id_type=pl.DeviceIdType.MESH,
        )
        copy.start()
        return copy

    def landed(ref, sem):
        pltpu.make_async_copy(ref, ref, sem).wait()

    barrier = pltpu.get_barrier_semaphore()
    greeted = [near(before, 0), near(before, 1), near(after, 0), near(after, 1), at_y[1], at_y[2], at_y[3], at_z, at_c]
    for where in greeted:
        pl.semaphore_signal(barrier, inc=1, device_id=where, device_id_type=pl.DeviceIdType.MESH)
    pl.semaphore_wait(barrier, len(greeted))

    sent = []
    for k in range(kpts):
        for zz in range(NZ):
            sent.append(send(coef_in.at[k], coef.at[k, z, y, c], pair_out.at[k, zz], pair_sem.at[k, z], near(before, zz)))
    own = pltpu.make_async_copy(coef_in.at[pl.ds(kpts, kpts)], coef.at[pl.ds(kpts, kpts), z, y, c], load_sem.at[0])
    own.start()
    sent.append(send(coef_in.at[pl.ds(kpts, kpts)], coef.at[pl.ds(kpts, kpts), z, y, c], cz_sem.at[1], cz_sem.at[0], at_z))
    load_zeta = pltpu.make_async_copy(zeta_in, zeta, load_sem.at[1])
    load_zeta.start()
    load_orb = pltpu.make_async_copy(orb_in, orb, load_sem.at[2])
    load_orb.start()

    def pair(ch, at):
        return coef.at[ch, :, at, c]

    def spread(ch):
        for n, where in enumerate((at_y[1], at_y[3], at_c)):
            sent.append(send(pair(ch, y), pair(ch, y), ag_out.at[ch, n], ag_sem.at[ch, n], where))

    def relay(ch):
        landed(pair(ch, ys[3]), ag_sem.at[ch, 0])
        one = coef.at[ch, 0, ys[3], c]
        sent.append(send(one, one, ag_out.at[ch, 3], ag_sem.at[ch, 3], at_y[1]))
        sent.append(send(pair(ch, ys[3]), pair(ch, ys[3]), ag_out.at[ch, 5], ag_sem.at[ch, 5], at_c))
        landed(pair(ch, ys[1]), ag_sem.at[ch, 1])
        one = coef.at[ch, 1, ys[1], c]
        sent.append(send(one, one, ag_out.at[ch, 4], ag_sem.at[ch, 4], at_y[3]))
        sent.append(send(pair(ch, ys[1]), pair(ch, ys[1]), ag_out.at[ch, 6], ag_sem.at[ch, 6], at_c))

    def far(ch):
        landed(coef.at[ch, 0, ys[2], c], ag_sem.at[ch, 3])
        landed(coef.at[ch, 1, ys[2], c], ag_sem.at[ch, 4])
        sent.append(send(pair(ch, ys[2]), pair(ch, ys[2]), ag_out.at[ch, 7], ag_sem.at[ch, 7], at_c))

    def joined(ch):
        for n, at in ((2, y), (5, ys[3]), (6, ys[1]), (7, ys[2])):
            landed(coef.at[ch, :, at, 1 - c], ag_sem.at[ch, n])

    def gather(chunks, first):
        for ch in chunks:
            first(ch)
            spread(ch)
        for ch in chunks:
            relay(ch)
        for ch in chunks:
            far(ch)
        for ch in chunks:
            joined(ch)

    def moved(ch):
        landed(coef.at[ch, 0, y, c], pair_sem.at[ch, 0])
        landed(coef.at[ch, 1, y, c], pair_sem.at[ch, 1])

    def product(ch, r):
        lines = zeta[pl.ds(pl.multiple_of(r * tile, tile), tile), :]
        return jnp.dot(lines, coef[ch].reshape(zeta.shape[1], -1), preferred_element_type=jnp.float32)

    def term(k):
        def step(r, carry):
            value = product(k, r)
            top = jnp.maximum(jnp.max(jnp.abs(value), axis=0, keepdims=True), 1e-30)
            level = jnp.round(value * (LEVELS / top)).astype(jnp.int32)
            psend[k, pl.ds(pl.multiple_of(r * tile, tile), tile), :] = level.astype(jnp.int16)
            ssend[k, r] = top / LEVELS
            return carry

        lax.fori_loop(0, tiles, step, 0)
        sent.append(send(psend.at[k], precv.at[k], p_out.at[k, 0], p_sem.at[k, 0], at_after))
        sent.append(send(ssend.at[k], srecv.at[k], p_out.at[k, 1], p_sem.at[k, 1], at_after))

    def own_term(k):
        def step(r, carry):
            field[k, pl.ds(pl.multiple_of(r * tile, tile), tile), :] = product(kpts + k, r)
            return carry

        lax.fori_loop(0, tiles, step, 0)

    stores = []

    def combine(k):
        landed(precv.at[k], p_sem.at[k, 0])
        landed(srecv.at[k], p_sem.at[k, 1])

        def step(r, carry):
            at = pl.ds(pl.multiple_of(r * tile, tile), tile)
            value = field[k, at, :] + precv[k, at, :].astype(jnp.int32).astype(jnp.float32) * srecv[k, r]
            field[k, at, :] = value
            high = value.astype(jnp.bfloat16)
            low = (value - high.astype(jnp.float32)).astype(jnp.bfloat16)
            lines = orb[k, at, :]
            over = (((0,), (0,)), ((), ()))
            added = lax.dot_general(lines, high, over, preferred_element_type=jnp.float32)
            added += lax.dot_general(lines, low, over, preferred_element_type=jnp.float32)
            added = added.reshape(part.shape[1:])

            @pl.when(r == 0)
            def _():
                part[k] = added

            @pl.when(r > 0)
            def _():
                part[k] += added

            return carry

        lax.fori_loop(0, tiles, step, 0)
        out = pltpu.make_async_copy(field.at[k], field_out.at[k], store_sem.at[0, k])
        out.start()
        stores.append(out)

    def reduce(k):
        sent.append(send(part.at[k, 1 - c], rsib.at[k], ar_out.at[k, 0], ar_sem.at[k, 0], at_c))
        landed(rsib.at[k], ar_sem.at[k, 0])
        half[k] = part[k, c] + rsib[k]
        for d in range(1, NY):
            sent.append(send(half.at[k, ys[d]], ry.at[k, d - 1], ar_out.at[k, d], ar_sem.at[k, d], at_y[d]))
        total = half[k, y]
        for d in range(1, NY):
            landed(ry.at[k, d - 1], ar_sem.at[k, d])
            total = total + ry[k, d - 1]
        quarter[k] = total
        sent.append(send(quarter.at[k], rz.at[k], ar_out.at[k, 4], ar_sem.at[k, 4], at_z))
        landed(rz.at[k], ar_sem.at[k, 4])
        final[k, c, y] = quarter[k] + rz[k]
        for d in range(1, NY):
            sent.append(send(final.at[k, c, y], final.at[k, c, y], ar_out.at[k, 4 + d], ar_sem.at[k, 4 + d], at_y[d]))
        for d in range(1, NY):
            landed(final.at[k, c, ys[NY - d]], ar_sem.at[k, 4 + d])
        sent.append(send(final.at[k, c], final.at[k, c], ar_out.at[k, 8], ar_sem.at[k, 8], at_c))
        landed(final.at[k, 1 - c], ar_sem.at[k, 8])
        out = pltpu.make_async_copy(final.at[k], inter_out.at[k], store_sem.at[1, k])
        out.start()
        stores.append(out)

    gather((0,), moved)
    load_zeta.wait()
    term(0)
    gather((1,), moved)
    term(1)
    gather((2, 3), moved)
    term(2)
    term(3)
    own.wait()
    landed(coef.at[pl.ds(kpts, kpts), 1 - z, y, c], cz_sem.at[0])
    gather((4, 5), lambda ch: None)
    own_term(0)
    own_term(1)
    load_orb.wait()
    combine(0)
    reduce(0)
    gather((6, 7), lambda ch: None)
    own_term(2)
    own_term(3)
    for k in range(1, kpts):
        combine(k)
        reduce(k)
    for copy in sent:
        copy.wait_send()
    for copy in stores:
        copy.wait()


def exchange(zeta, coefs, orbitals):
    rows, points = zeta.shape
    kpts, _, bands = orbitals.shape
    tile = min(TILE, rows)
    share = coefs.shape[1]
    slice_ = bands // (NC * NY)
    f32, bf16, i16 = jnp.float32, jnp.bfloat16, jnp.int16
    anywhere = pl.BlockSpec(memory_space=pltpu.HBM)
    dma = pltpu.SemaphoreType.DMA
    return pl.pallas_call(
        kernel,
        out_shape=(
            jax.ShapeDtypeStruct((kpts, rows, bands), f32),
            jax.ShapeDtypeStruct((kpts, NC, NY, slice_, bands), f32),
        ),
        in_specs=[anywhere] * 3,
        out_specs=(anywhere, anywhere),
        scratch_shapes=[
            pltpu.VMEM((rows, points), bf16),
            pltpu.VMEM((2 * kpts, NZ, NY, NC, share, bands), bf16),
            pltpu.VMEM((kpts, rows, bands), bf16),
            pltpu.VMEM((kpts, rows, bands), i16),
            pltpu.VMEM((kpts, rows, bands), i16),
            pltpu.VMEM((kpts, rows // tile, 1, bands), f32),
            pltpu.VMEM((kpts, rows // tile, 1, bands), f32),
            pltpu.VMEM((kpts, rows, bands), f32),
            pltpu.VMEM((kpts, NC, NY, slice_, bands), f32),
            pltpu.VMEM((kpts, NY, slice_, bands), f32),
            pltpu.VMEM((kpts, NY, slice_, bands), f32),
            pltpu.VMEM((kpts, NY - 1, slice_, bands), f32),
            pltpu.VMEM((kpts, slice_, bands), f32),
            pltpu.VMEM((kpts, slice_, bands), f32),
            pltpu.VMEM((kpts, NC, NY, slice_, bands), f32),
            dma((3,)),
            dma((kpts, NZ)),
            dma((kpts, NZ)),
            dma((2,)),
            dma((2 * kpts, 8)),
            dma((2 * kpts, 8)),
            dma((kpts, 2)),
            dma((kpts, 2)),
            dma((kpts, 9)),
            dma((kpts, 9)),
            dma((2, kpts)),
        ],
        compiler_params=pltpu.CompilerParams(collective_id=0, has_side_effects=True, vmem_limit_bytes=60 * 1024 * 1024),
        name="exchange",
    )(zeta, coefs, orbitals)


def on_device(zeta_sets, coef_blocks, pair_table, band_counts, orbitals):
    swap = (pair_table[:, :1] == 1)[:, :, None]
    columns = jnp.arange(coef_blocks.shape[3], dtype=jnp.int32)
    keep = columns[None, :] < band_counts[:, None]
    zero = jnp.zeros((), jnp.bfloat16)
    straight, crossed = coef_blocks[:, 0], coef_blocks[:, 1]
    nearest = jnp.where(keep[:, None, :], jnp.where(swap, crossed, straight), zero)
    previous = jnp.where(keep[:, None, :], jnp.where(swap, straight, crossed), zero)
    coefs = jnp.concatenate([previous, nearest], axis=0)
    fields, intersection = exchange(zeta_sets[0], coefs, orbitals)
    kpts, bands = keep.shape
    intersection = intersection.reshape(kpts, bands, bands)
    intersection = jnp.where(keep[:, :, None], intersection, jnp.zeros((), jnp.float32))
    return fields, intersection


def solution(mesh):
    return jax.shard_map(
        on_device,
        mesh=mesh,
        in_specs=(
            P("blk", "slab", None),
            P("blk", None, "slab", None),
            P("blk", None),
            P("blk"),
            P("blk", "slab", None),
        ),
        out_specs=(P("blk", "slab", None), P("blk", None, None)),
        check_vma=False,
    )
```

```python
import functools

import jax
import jax.numpy as jnp
from jax import lax
from jax.experimental import pallas as pl
from jax.experimental.pallas import tpu as pltpu
from jax.sharding import PartitionSpec as P

NZ, NY, NC = 2, 4, 2
LEVELS = 32767.0
TILE = 256
SPLIT_Z = 4
RELAY = (0, 12, 11, 0)
RELAY_UNIT = 32


def slab_at(z, y, c):
    return (z * NY + y) * NC + c


def kernel(
    pair_table, counts, zeta_in, coef_in, orb_in, field, final,
    zeta, raw, picked, coef, orb, psend, precv, middle, ssend, srecv,
    part, rsib, half, ry, quarter, rz,
    load_sem, pair_sem, pair_out, cz_sem, ag_sem, ag_out, p_sem, p_out, relay_sem, relay_out, ar_sem, ar_out,
):
    kpts, rows, bands = field.shape
    tile = min(TILE, rows)
    tiles = rows // tile
    blk, slab = lax.axis_index("blk"), lax.axis_index("slab")
    nblk = lax.axis_size("blk")
    nx, nz = nblk // SPLIT_Z, NZ * SPLIT_Z
    c = lax.rem(slab, NC)
    y = lax.rem(slab // NC, NY)
    z = slab // (NC * NY)
    x = blk // SPLIT_Z
    height = lax.rem(blk, SPLIT_Z) * NZ + z
    after, before = lax.rem(blk + 1, nblk), lax.rem(blk + nblk - 1, nblk)
    ys = [lax.rem(y + d, NY) for d in range(NY)]
    at_y = [{"slab": slab_at(z, ys[d], c)} for d in range(NY)]
    at_z = {"slab": slab_at(1 - z, y, c)}
    at_c = {"slab": slab_at(z, y, 1 - c)}
    at_after = {"blk": after, "slab": slab}

    def near(other, zz):
        return {"blk": other, "slab": slab_at(zz, y, c)}

    def up(xx, level):
        level = lax.rem(level, nz)
        return {"blk": lax.rem(xx, nx) * SPLIT_Z + level // NZ, "slab": slab_at(lax.rem(level, NZ), y, c)}

    def crossing(level):
        return (lax.rem(level, nz) + NZ) // nz

    below, above = height + nz - 3, height + 3
    relay_to, relay_from = up(x, below), up(x, above)
    forward_to = up(x + crossing(above), below)
    forward_from = up(x + nx - crossing(height + nz - NZ), above)

    def send(src, dst, out, arrived, where):
        copy = pltpu.make_async_remote_copy(
            src_ref=src, dst_ref=dst, send_sem=out, recv_sem=arrived,
            device_id=where, device_id_type=pl.DeviceIdType.MESH,
        )
        copy.start()
        sent.append(copy)

    def landed(ref, sem):
        pltpu.make_async_copy(ref, ref, sem).wait()

    sent = []
    load_raw = pltpu.make_async_copy(coef_in, raw, load_sem.at[0])
    load_raw.start()
    load_zeta = pltpu.make_async_copy(zeta_in, zeta, load_sem.at[1])
    load_zeta.start()
    load_orb = pltpu.make_async_copy(orb_in, orb, load_sem.at[2])
    load_orb.start()
    barrier = pltpu.get_barrier_semaphore()
    greeted = [
        near(before, 0), near(before, 1), near(after, 0), near(after, 1), at_y[1], at_y[2], at_y[3], at_z, at_c,
        relay_to, relay_from, forward_to, forward_from,
    ]
    for where in greeted:
        pl.semaphore_signal(barrier, inc=1, device_id=where, device_id_type=pl.DeviceIdType.MESH)
    load_raw.wait()
    for k in range(kpts):
        swap = jnp.full(raw.shape[2:], pair_table[0, k], jnp.int32) == 1
        one, two = raw[k, 0], raw[k, 1]
        picked[k] = jnp.where(swap, one, two)
        near_set = jnp.where(swap, two, one)
        picked[kpts + k] = near_set
        coef[kpts + k, z, y, c] = near_set
    pl.semaphore_wait(barrier, len(greeted))

    wide, narrow = pl.ds(0, bands), bands // 2
    pieces = [(0, pl.ds(0, narrow)), (0, pl.ds(narrow, narrow))] + [(k, wide) for k in range(1, kpts)]
    for n, (k, cols) in enumerate(pieces):
        for zz in range(NZ):
            send(picked.at[k, :, cols], coef.at[k, z, y, c, :, cols], pair_out.at[n, zz], pair_sem.at[n, z], near(before, zz))
    nearest = pl.ds(kpts, kpts)
    send(picked.at[nearest], coef.at[nearest, z, y, c], cz_sem.at[1], cz_sem.at[0], at_z)

    def view(n, at, cc):
        if n == len(pieces):
            return coef.at[nearest, :, at, cc]
        return coef.at[pieces[n][0], :, at, cc, :, pieces[n][1]]

    def spread(n):
        for lane, where in enumerate((at_y[1], at_y[3], at_y[2], at_c)):
            send(view(n, y, c), view(n, y, c), ag_out.at[n, lane], ag_sem.at[n, lane], where)

    def pass_on(n):
        for lane, at in enumerate((ys[3], ys[1], ys[2])):
            landed(view(n, at, c), ag_sem.at[n, lane])
            send(view(n, at, c), view(n, at, c), ag_out.at[n, 4 + lane], ag_sem.at[n, 4 + lane], at_c)

    def joined(n):
        for lane, at in ((3, y), (4, ys[3]), (5, ys[1]), (6, ys[2])):
            landed(view(n, at, 1 - c), ag_sem.at[n, lane])

    def moved(n):
        k, cols = pieces[n]
        for zz in range(NZ):
            landed(coef.at[k, zz, y, c, :, cols], pair_sem.at[n, zz])

    def begin(n):
        if n == len(pieces):
            landed(coef.at[nearest, 1 - z, y, c], cz_sem.at[0])
        else:
            moved(n)
        spread(n)

    def product(ch, r, cols):
        lines = zeta[pl.ds(pl.multiple_of(r * tile, tile), tile), :]
        block = coef[ch, :, :, :, :, cols]
        return jnp.dot(lines, block.reshape(zeta.shape[1], block.shape[-1]), preferred_element_type=jnp.float32)

    def extra(k):
        return rows * RELAY[k] // RELAY_UNIT

    def parts(k):
        return pl.ds(0, rows - extra(k)), pl.ds(rows - extra(k), extra(k))

    def term(n):
        k, cols = pieces[n]

        def step(r, carry):
            value = product(k, r, cols)
            top = jnp.maximum(jnp.max(jnp.abs(value), axis=0, keepdims=True), 1e-30)
            level = jnp.round(value * (LEVELS / top)).astype(jnp.int32)
            psend[k, pl.ds(pl.multiple_of(r * tile, tile), tile), cols] = level.astype(jnp.int16)
            ssend[k, r, :, cols] = top / LEVELS
            return carry

        lax.fori_loop(0, tiles, step, 0)
        direct, other = parts(k)
        if extra(k):
            send(psend.at[k, other], middle.at[k, pl.ds(0, extra(k))], relay_out.at[k, 0], relay_sem.at[k, 0], relay_to)
        send(ssend.at[k, :, :, cols], srecv.at[k, :, :, cols], p_out.at[n, 1], p_sem.at[n, 1], at_after)
        send(psend.at[k, direct, cols], precv.at[k, direct, cols], p_out.at[n, 0], p_sem.at[n, 0], at_after)

    def forward(k):
        if extra(k):
            held = middle.at[k, pl.ds(0, extra(k))]
            landed(held, relay_sem.at[k, 0])
            send(held, precv.at[k, parts(k)[1]], relay_out.at[k, 1], relay_sem.at[k, 1], forward_to)

    def own_term(k):
        def step(r, carry):
            field[k, pl.ds(pl.multiple_of(r * tile, tile), tile), :] = product(kpts + k, r, wide)
            return carry

        lax.fori_loop(0, tiles, step, 0)

    def arrived(k):
        direct, other = parts(k)
        for n, (owner, cols) in enumerate(pieces):
            if owner == k:
                landed(precv.at[k, direct, cols], p_sem.at[n, 0])
                landed(srecv.at[k, :, :, cols], p_sem.at[n, 1])
        if extra(k):
            landed(precv.at[k, other], relay_sem.at[k, 1])

    def combine(k):
        keep = lax.broadcasted_iota(jnp.int32, (1, bands), 1) < counts[k]
        weight = jnp.where(keep, 1.0, 0.0)
        weight_low = weight.astype(jnp.bfloat16)

        def step(r, carry):
            at = pl.ds(pl.multiple_of(r * tile, tile), tile)
            value = field[k, at, :] + precv[k, at, :].astype(jnp.int32).astype(jnp.float32) * srecv[k, r]
            value = value * weight
            field[k, at, :] = value
            high = value.astype(jnp.bfloat16)
            low = (value - high.astype(jnp.float32)).astype(jnp.bfloat16)
            lines = orb[k, at, :] * weight_low
            over = (((0,), (0,)), ((), ()))
            added = lax.dot_general(lines, high, over, preferred_element_type=jnp.float32)
            added += lax.dot_general(lines, low, over, preferred_element_type=jnp.float32)
            added = added.reshape(part.shape[1:])

            @pl.when(r == 0)
            def _():
                part[k] = added

            @pl.when(r > 0)
            def _():
                part[k] += added

            return carry

        lax.fori_loop(0, tiles, step, 0)
        send(part.at[k, 1 - c], rsib.at[k], ar_out.at[k, 0], ar_sem.at[k, 0], at_c)

    def scatter_y(k):
        landed(rsib.at[k], ar_sem.at[k, 0])
        half[k] = part[k, c] + rsib[k]
        for d in range(1, NY):
            send(half.at[k, ys[d]], ry.at[k, d - 1], ar_out.at[k, d], ar_sem.at[k, d], at_y[d])

    def swap_z(k):
        total = half[k, y]
        for d in range(1, NY):
            landed(ry.at[k, d - 1], ar_sem.at[k, d])
            total = total + ry[k, d - 1]
        quarter[k] = total
        send(quarter.at[k], rz.at[k], ar_out.at[k, 4], ar_sem.at[k, 4], at_z)

    def gather_y(k):
        landed(rz.at[k], ar_sem.at[k, 4])
        final[k, c, y] = quarter[k] + rz[k]
        for d in range(1, NY):
            send(final.at[k, c, y], final.at[k, c, y], ar_out.at[k, 4 + d], ar_sem.at[k, 4 + d], at_y[d])

    def gather_c(k):
        for d in range(1, NY):
            landed(final.at[k, c, ys[NY - d]], ar_sem.at[k, 4 + d])
        send(final.at[k, c], final.at[k, c], ar_out.at[k, 8], ar_sem.at[k, 8], at_c)

    def settle(k):
        landed(final.at[k, 1 - c], ar_sem.at[k, 8])

    begin(0)
    load_zeta.wait()
    for n in range(len(pieces)):
        pass_on(n)
        begin(n + 1)
        joined(n)
        term(n)
    forward(1)
    pass_on(5)
    forward(2)
    joined(5)
    for k in range(kpts):
        own_term(k)
    load_orb.wait()
    for k in range(3):
        arrived(k)
        combine(k)
    for k in range(3):
        scatter_y(k)
    for k in range(3):
        swap_z(k)
    arrived(3)
    combine(3)
    scatter_y(3)
    for k in range(3):
        gather_y(k)
    swap_z(3)
    gather_y(3)
    for k in range(kpts):
        gather_c(k)
    for k in range(kpts):
        settle(k)
    for copy in sent:
        copy.wait_send()


def exchange(zeta, coefs, orbitals, pair_table, counts):
    rows, points = zeta.shape
    kpts, _, share, bands = coefs.shape
    tile = min(TILE, rows)
    slice_ = bands // (NC * NY)
    f32, bf16, i16 = jnp.float32, jnp.bfloat16, jnp.int16
    hbm = pl.BlockSpec(memory_space=pltpu.HBM)
    smem = pl.BlockSpec(memory_space=pltpu.SMEM)
    vmem = pl.BlockSpec(memory_space=pltpu.VMEM)
    dma = pltpu.SemaphoreType.DMA
    most = rows * max(max(RELAY), 1) // RELAY_UNIT
    shapes = ((kpts, rows, bands), (kpts, NC, NY, slice_, bands))
    return pl.pallas_call(
        kernel,
        out_shape=tuple(pltpu.VMEM(shape, f32) for shape in shapes),
        in_specs=[smem, smem, hbm, hbm, hbm],
        out_specs=(vmem, vmem),
        scratch_shapes=[
            pltpu.VMEM((rows, points), bf16),
            pltpu.VMEM((kpts, 2, share, bands), bf16),
            pltpu.VMEM((2 * kpts, share, bands), bf16),
            pltpu.VMEM((2 * kpts, NZ, NY, NC, share, bands), bf16),
            pltpu.VMEM((kpts, rows, bands), bf16),
            pltpu.VMEM((kpts, rows, bands), i16),
            pltpu.VMEM((kpts, rows, bands), i16),
            pltpu.VMEM((kpts, most, bands), i16),
            pltpu.VMEM((kpts, rows // tile, 1, bands), f32),
            pltpu.VMEM((kpts, rows // tile, 1, bands), f32),
            pltpu.VMEM((kpts, NC, NY, slice_, bands), f32),
            pltpu.VMEM((kpts, NY, slice_, bands), f32),
            pltpu.VMEM((kpts, NY, slice_, bands), f32),
            pltpu.VMEM((kpts, NY - 1, slice_, bands), f32),
            pltpu.VMEM((kpts, slice_, bands), f32),
            pltpu.VMEM((kpts, slice_, bands), f32),
            dma((3,)),
            dma((kpts + 1, NZ)),
            dma((kpts + 1, NZ)),
            dma((2,)),
            dma((kpts + 2, 7)),
            dma((kpts + 2, 7)),
            dma((kpts + 1, 2)),
            dma((kpts + 1, 2)),
            dma((kpts, 2)),
            dma((kpts, 2)),
            dma((kpts, 9)),
            dma((kpts, 9)),
        ],
        compiler_params=pltpu.CompilerParams(collective_id=0, has_side_effects=True, vmem_limit_bytes=61_700_000),
        name="exchange",
    )(pair_table.T, counts, zeta, coefs, orbitals)


def on_device(zeta_sets, coef_blocks, pair_table, band_counts, orbitals):
    fields, intersection = exchange(zeta_sets[0], coef_blocks, orbitals, pair_table, band_counts)
    kpts, bands = fields.shape[0], fields.shape[2]
    return fields, intersection.reshape(kpts, bands, bands)


def solution(mesh):
    return jax.shard_map(
        on_device,
        mesh=mesh,
        in_specs=(
            P("blk", "slab", None),
            P("blk", None, "slab", None),
            P("blk", None),
            P("blk"),
            P("blk", "slab", None),
        ),
        out_specs=(P("blk", "slab", None), P("blk", None, None)),
        check_vma=False,
    )
```

```python
import functools

import jax
import jax.numpy as jnp
from jax import lax
from jax.experimental import pallas as pl
from jax.experimental.pallas import tpu as pltpu
from jax.sharding import PartitionSpec as P

NZ, NY, NC = 2, 4, 2
LEVELS = 32767.0
TILE = 256
SPLIT_Z = 4
RELAY = (0, 12, 11, 0)
RELAY_UNIT = 32


def slab_at(z, y, c):
    return (z * NY + y) * NC + c


def kernel(
    pair_table, counts, zeta_in, coef_in, orb_in, field, final,
    zeta, raw, picked, coef, orb, psend, precv, middle, ssend, srecv,
    part, rsib, half, ry, quarter, rz,
    load_sem, pair_sem, pair_out, cz_sem, ag_sem, ag_out, p_sem, p_out, relay_sem, relay_out, ar_sem, ar_out,
):
    kpts, rows, bands = field.shape
    tile = min(TILE, rows)
    tiles = rows // tile
    blk, slab = lax.axis_index("blk"), lax.axis_index("slab")
    nblk = lax.axis_size("blk")
    nx, nz = nblk // SPLIT_Z, NZ * SPLIT_Z
    c = lax.rem(slab, NC)
    y = lax.rem(slab // NC, NY)
    z = slab // (NC * NY)
    x = blk // SPLIT_Z
    height = lax.rem(blk, SPLIT_Z) * NZ + z
    after, before = lax.rem(blk + 1, nblk), lax.rem(blk + nblk - 1, nblk)
    ys = [lax.rem(y + d, NY) for d in range(NY)]
    at_y = [{"slab": slab_at(z, ys[d], c)} for d in range(NY)]
    at_z = {"slab": slab_at(1 - z, y, c)}
    at_c = {"slab": slab_at(z, y, 1 - c)}
    at_after = {"blk": after, "slab": slab}

    def near(other, zz):
        return {"blk": other, "slab": slab_at(zz, y, c)}

    def up(xx, level):
        level = lax.rem(level, nz)
        return {"blk": lax.rem(xx, nx) * SPLIT_Z + level // NZ, "slab": slab_at(lax.rem(level, NZ), y, c)}

    def crossing(level):
        return (lax.rem(level, nz) + NZ) // nz

    below, above = height + nz - 3, height + 3
    relay_to, relay_from = up(x, below), up(x, above)
    forward_to = up(x + crossing(above), below)
    forward_from = up(x + nx - crossing(height + nz - NZ), above)

    def send(src, dst, out, arrived, where):
        copy = pltpu.make_async_remote_copy(
            src_ref=src, dst_ref=dst, send_sem=out, recv_sem=arrived,
            device_id=where, device_id_type=pl.DeviceIdType.MESH,
        )
        copy.start()
        sent.append(copy)

    def landed(ref, sem):
        pltpu.make_async_copy(ref, ref, sem).wait()

    sent = []
    load_raw = pltpu.make_async_copy(coef_in, raw, load_sem.at[0])
    load_raw.start()
    load_zeta = pltpu.make_async_copy(zeta_in, zeta, load_sem.at[1])
    load_zeta.start()
    load_orb = pltpu.make_async_copy(orb_in, orb, load_sem.at[2])
    load_orb.start()
    barrier = pltpu.get_barrier_semaphore()
    greeted = [
        near(before, 0), near(before, 1), near(after, 0), near(after, 1), at_y[1], at_y[2], at_y[3], at_z, at_c,
        relay_to, relay_from, forward_to, forward_from,
    ]
    for where in greeted:
        pl.semaphore_signal(barrier, inc=1, device_id=where, device_id_type=pl.DeviceIdType.MESH)
    load_raw.wait()
    for k in range(kpts):
        swap = jnp.full(raw.shape[2:], pair_table[0, k], jnp.int32) == 1
        one, two = raw[k, 0], raw[k, 1]
        picked[k] = jnp.where(swap, one, two)
        near_set = jnp.where(swap, two, one)
        picked[kpts + k] = near_set
        coef[kpts + k, z, y, c] = near_set
    pl.semaphore_wait(barrier, len(greeted))

    wide, narrow = pl.ds(0, bands), bands // 2
    halves = (pl.ds(0, narrow), pl.ds(narrow, narrow))
    last = kpts - 1
    pieces = [(0, cols) for cols in halves] + [(k, wide) for k in range(1, last)] + [(last, cols) for cols in halves]
    units = [(k, wide) for k in range(last)] + [(last, cols) for cols in halves]
    for n, (k, cols) in enumerate(pieces):
        for zz in range(NZ):
            send(picked.at[k, :, cols], coef.at[k, z, y, c, :, cols], pair_out.at[n, zz], pair_sem.at[n, z], near(before, zz))
    nearest, pack = pl.ds(kpts, kpts), kpts // 2
    send(picked.at[nearest], coef.at[nearest, z, y, c], cz_sem.at[1], cz_sem.at[0], at_z)

    def view(n, at, cc):
        if n >= len(pieces):
            return coef.at[pl.ds(kpts + (n - len(pieces)) * pack, pack), :, at, cc]
        return coef.at[pieces[n][0], :, at, cc, :, pieces[n][1]]

    def spread(n):
        for lane, where in enumerate((at_y[1], at_y[3], at_y[2], at_c)):
            send(view(n, y, c), view(n, y, c), ag_out.at[n, lane], ag_sem.at[n, lane], where)

    def pass_on(n):
        for lane, at in enumerate((ys[3], ys[1], ys[2])):
            landed(view(n, at, c), ag_sem.at[n, lane])
            send(view(n, at, c), view(n, at, c), ag_out.at[n, 4 + lane], ag_sem.at[n, 4 + lane], at_c)

    def joined(n):
        for lane, at in ((3, y), (4, ys[3]), (5, ys[1]), (6, ys[2])):
            landed(view(n, at, 1 - c), ag_sem.at[n, lane])

    def moved(n):
        k, cols = pieces[n]
        for zz in range(NZ):
            landed(coef.at[k, zz, y, c, :, cols], pair_sem.at[n, zz])

    def begin(n):
        if n == len(pieces):
            landed(coef.at[nearest, 1 - z, y, c], cz_sem.at[0])
        elif n < len(pieces):
            moved(n)
        spread(n)

    def product(ch, r, cols):
        lines = zeta[pl.ds(pl.multiple_of(r * tile, tile), tile), :]
        block = coef[ch, :, :, :, :, cols]
        return jnp.dot(lines, block.reshape(zeta.shape[1], block.shape[-1]), preferred_element_type=jnp.float32)

    def extra(k):
        return rows * RELAY[k] // RELAY_UNIT

    def parts(k):
        return pl.ds(0, rows - extra(k)), pl.ds(rows - extra(k), extra(k))

    def term(n):
        k, cols = pieces[n]

        def step(r, carry):
            value = product(k, r, cols)
            top = jnp.maximum(jnp.max(jnp.abs(value), axis=0, keepdims=True), 1e-30)
            level = jnp.round(value * (LEVELS / top)).astype(jnp.int32)
            psend[k, pl.ds(pl.multiple_of(r * tile, tile), tile), cols] = level.astype(jnp.int16)
            ssend[k, r, :, cols] = top / LEVELS
            return carry

        direct, other = parts(k)
        if n == 0:
            for side in range(2):
                lax.fori_loop(side * tiles // 2, (side + 1) * tiles // 2, step, 0)
                some = pl.ds(side * rows // 2, rows // 2)
                send(psend.at[k, some, cols], precv.at[k, some, cols], p_out.at[n, 2 * side], p_sem.at[n, 2 * side], at_after)
        else:
            lax.fori_loop(0, tiles, step, 0)
            if extra(k):
                send(psend.at[k, other], middle.at[k, pl.ds(0, extra(k))], relay_out.at[k, 0], relay_sem.at[k, 0], relay_to)
            send(psend.at[k, direct, cols], precv.at[k, direct, cols], p_out.at[n, 0], p_sem.at[n, 0], at_after)
        send(ssend.at[k, :, :, cols], srecv.at[k, :, :, cols], p_out.at[n, 1], p_sem.at[n, 1], at_after)

    def forward(k):
        if extra(k):
            held = middle.at[k, pl.ds(0, extra(k))]
            landed(held, relay_sem.at[k, 0])
            send(held, precv.at[k, parts(k)[1]], relay_out.at[k, 1], relay_sem.at[k, 1], forward_to)

    def own_term(k):
        def step(r, carry):
            field[k, pl.ds(pl.multiple_of(r * tile, tile), tile), :] = product(kpts + k, r, wide)
            return carry

        lax.fori_loop(0, tiles, step, 0)

    def arrived(u):
        k, wanted = units[u]
        direct, other = parts(k)
        for n, (owner, cols) in enumerate(pieces):
            if owner != k or wanted not in (wide, cols):
                continue
            if n == 0:
                for side in range(2):
                    landed(precv.at[k, pl.ds(side * rows // 2, rows // 2), cols], p_sem.at[n, 2 * side])
            else:
                landed(precv.at[k, direct, cols], p_sem.at[n, 0])
            landed(srecv.at[k, :, :, cols], p_sem.at[n, 1])
        if extra(k):
            landed(precv.at[k, other], relay_sem.at[k, 1])

    def combine(u):
        k, cols = units[u]
        lane = lax.broadcasted_iota(jnp.int32, (1, bands), 1)
        weight = jnp.where(lane[:, : cols.size] + cols.start < counts[k], 1.0, 0.0)
        weight_low = jnp.where(lane < counts[k], 1.0, 0.0).astype(jnp.bfloat16)

        def step(r, carry):
            at = pl.ds(pl.multiple_of(r * tile, tile), tile)
            level = precv[k, at, cols].astype(jnp.int32).astype(jnp.float32)
            value = (field[k, at, cols] + level * srecv[k, r, :, cols]) * weight
            field[k, at, cols] = value
            high = value.astype(jnp.bfloat16)
            low = (value - high.astype(jnp.float32)).astype(jnp.bfloat16)
            lines = orb[k, at, :] * weight_low
            over = (((0,), (0,)), ((), ()))
            added = lax.dot_general(lines, high, over, preferred_element_type=jnp.float32)
            added += lax.dot_general(lines, low, over, preferred_element_type=jnp.float32)
            added = added.reshape(*part.shape[1:4], cols.size)

            @pl.when(r == 0)
            def _():
                part[k, :, :, :, cols] = added

            @pl.when(r > 0)
            def _():
                part[k, :, :, :, cols] += added

            return carry

        lax.fori_loop(0, tiles, step, 0)
        send(part.at[k, 1 - c, :, :, cols], rsib.at[k, :, :, cols], ar_out.at[u, 0], ar_sem.at[u, 0], at_c)

    def scatter_y(u):
        k, cols = units[u]
        landed(rsib.at[k, :, :, cols], ar_sem.at[u, 0])
        half[k, :, :, cols] = part[k, c, :, :, cols] + rsib[k, :, :, cols]
        for d in range(1, NY):
            send(half.at[k, ys[d], :, cols], ry.at[k, d - 1, :, cols], ar_out.at[u, d], ar_sem.at[u, d], at_y[d])

    def swap_z(u):
        k, cols = units[u]
        total = half[k, y, :, cols]
        for d in range(1, NY):
            landed(ry.at[k, d - 1, :, cols], ar_sem.at[u, d])
            total = total + ry[k, d - 1, :, cols]
        quarter[k, :, cols] = total
        send(quarter.at[k, :, cols], rz.at[k, :, cols], ar_out.at[u, 4], ar_sem.at[u, 4], at_z)

    def gather_y(u):
        k, cols = units[u]
        landed(rz.at[k, :, cols], ar_sem.at[u, 4])
        final[k, c, y, :, cols] = quarter[k, :, cols] + rz[k, :, cols]
        done = final.at[k, c, y, :, cols]
        for d in range(1, NY):
            send(done, done, ar_out.at[u, 4 + d], ar_sem.at[u, 4 + d], at_y[d])

    def gather_c(u):
        k, cols = units[u]
        for d in range(1, NY):
            landed(final.at[k, c, ys[NY - d], :, cols], ar_sem.at[u, 4 + d])
        done = final.at[k, c, :, :, cols]
        send(done, done, ar_out.at[u, 8], ar_sem.at[u, 8], at_c)

    def settle(u):
        k, cols = units[u]
        landed(final.at[k, 1 - c, :, :, cols], ar_sem.at[u, 8])

    begin(0)
    load_zeta.wait()
    for n in range(len(pieces)):
        pass_on(n)
        begin(n + 1)
        joined(n)
        term(n)
    begin(7)
    forward(1)
    pass_on(6)
    forward(2)
    joined(6)
    own_term(0)
    own_term(1)
    load_orb.wait()
    arrived(0)
    combine(0)
    pass_on(7)
    scatter_y(0)
    joined(7)
    own_term(2)
    arrived(1)
    combine(1)
    swap_z(0)
    own_term(3)
    scatter_y(1)
    arrived(2)
    combine(2)
    swap_z(1)
    scatter_y(2)
    arrived(3)
    combine(3)
    swap_z(2)
    scatter_y(3)
    arrived(4)
    combine(4)
    swap_z(3)
    scatter_y(4)
    for u in range(4):
        gather_y(u)
    swap_z(4)
    gather_y(4)
    for u in range(5):
        gather_c(u)
    for u in range(5):
        settle(u)
    for copy in sent:
        copy.wait_send()


def exchange(zeta, coefs, orbitals, pair_table, counts):
    rows, points = zeta.shape
    kpts, _, share, bands = coefs.shape
    tile = min(TILE, rows)
    slice_ = bands // (NC * NY)
    f32, bf16, i16 = jnp.float32, jnp.bfloat16, jnp.int16
    hbm = pl.BlockSpec(memory_space=pltpu.HBM)
    smem = pl.BlockSpec(memory_space=pltpu.SMEM)
    vmem = pl.BlockSpec(memory_space=pltpu.VMEM)
    dma = pltpu.SemaphoreType.DMA
    most = rows * max(max(RELAY), 1) // RELAY_UNIT
    shapes = ((kpts, rows, bands), (kpts, NC, NY, slice_, bands))
    return pl.pallas_call(
        kernel,
        out_shape=tuple(pltpu.VMEM(shape, f32) for shape in shapes),
        in_specs=[smem, smem, hbm, hbm, hbm],
        out_specs=(vmem, vmem),
        scratch_shapes=[
            pltpu.VMEM((rows, points), bf16),
            pltpu.VMEM((kpts, 2, share, bands), bf16),
            pltpu.VMEM((2 * kpts, share, bands), bf16),
            pltpu.VMEM((2 * kpts, NZ, NY, NC, share, bands), bf16),
            pltpu.VMEM((kpts, rows, bands), bf16),
            pltpu.VMEM((kpts, rows, bands), i16),
            pltpu.VMEM((kpts, rows, bands), i16),
            pltpu.VMEM((kpts, most, bands), i16),
            pltpu.VMEM((kpts, rows // tile, 1, bands), f32),
            pltpu.VMEM((kpts, rows // tile, 1, bands), f32),
            pltpu.VMEM((kpts, NC, NY, slice_, bands), f32),
            pltpu.VMEM((kpts, NY, slice_, bands), f32),
            pltpu.VMEM((kpts, NY, slice_, bands), f32),
            pltpu.VMEM((kpts, NY - 1, slice_, bands), f32),
            pltpu.VMEM((kpts, slice_, bands), f32),
            pltpu.VMEM((kpts, slice_, bands), f32),
            dma((3,)),
            dma((kpts + 2, NZ)),
            dma((kpts + 2, NZ)),
            dma((2,)),
            dma((kpts + 4, 7)),
            dma((kpts + 4, 7)),
            dma((kpts + 2, 3)),
            dma((kpts + 2, 3)),
            dma((kpts, 2)),
            dma((kpts, 2)),
            dma((kpts + 1, 9)),
            dma((kpts + 1, 9)),
        ],
        compiler_params=pltpu.CompilerParams(collective_id=0, has_side_effects=True, vmem_limit_bytes=61_700_000),
        name="exchange",
    )(pair_table.T, counts, zeta, coefs, orbitals)


def on_device(zeta_sets, coef_blocks, pair_table, band_counts, orbitals):
    fields, intersection = exchange(zeta_sets[0], coef_blocks, orbitals, pair_table, band_counts)
    kpts, bands = fields.shape[0], fields.shape[2]
    return fields, intersection.reshape(kpts, bands, bands)


def solution(mesh):
    return jax.shard_map(
        on_device,
        mesh=mesh,
        in_specs=(
            P("blk", "slab", None),
            P("blk", None, "slab", None),
            P("blk", None),
            P("blk"),
            P("blk", "slab", None),
        ),
        out_specs=(P("blk", "slab", None), P("blk", None, None)),
        check_vma=False,
    )
```

```python
import functools

import jax
import jax.numpy as jnp
from jax import lax
from jax.experimental import pallas as pl
from jax.experimental.pallas import tpu as pltpu
from jax.sharding import PartitionSpec as P

NZ, NY, NC = 2, 4, 2
LEVELS = 32767.0
TILE = 256
SPLIT_Z = 4
RELAY = (0, 12, 11, 0)
RELAY_UNIT = 32


def slab_at(z, y, c):
    return (z * NY + y) * NC + c


def kernel(
    table_in, counts_in, zeta_in, coef_in, orb_in, field, final,
    pair_table, counts, zeta, raw, picked, coef, orb, psend, precv, middle, ssend, srecv,
    part, rsib, half, ry, quarter, rz,
    load_sem, pair_sem, pair_out, cz_sem, ag_sem, ag_out, p_sem, p_out, relay_sem, relay_out, ar_sem, ar_out,
):
    kpts, rows, bands = field.shape
    tile = min(TILE, rows)
    tiles = rows // tile
    blk, slab = lax.axis_index("blk"), lax.axis_index("slab")
    nblk = lax.axis_size("blk")
    nx, nz = nblk // SPLIT_Z, NZ * SPLIT_Z
    c = lax.rem(slab, NC)
    y = lax.rem(slab // NC, NY)
    z = slab // (NC * NY)
    x = blk // SPLIT_Z
    height = lax.rem(blk, SPLIT_Z) * NZ + z
    after, before = lax.rem(blk + 1, nblk), lax.rem(blk + nblk - 1, nblk)
    ys = [lax.rem(y + d, NY) for d in range(NY)]
    at_y = [{"slab": slab_at(z, ys[d], c)} for d in range(NY)]
    at_z = {"slab": slab_at(1 - z, y, c)}
    at_c = {"slab": slab_at(z, y, 1 - c)}
    at_after = {"blk": after, "slab": slab}

    def near(other, zz):
        return {"blk": other, "slab": slab_at(zz, y, c)}

    def up(xx, level):
        level = lax.rem(level, nz)
        return {"blk": lax.rem(xx, nx) * SPLIT_Z + level // NZ, "slab": slab_at(lax.rem(level, NZ), y, c)}

    def crossing(level):
        return (lax.rem(level, nz) + NZ) // nz

    below, above = height + nz - 3, height + 3
    relay_to, relay_from = up(x, below), up(x, above)
    forward_to = up(x + crossing(above), below)
    forward_from = up(x + nx - crossing(height + nz - NZ), above)

    def send(src, dst, out, arrived, where):
        copy = pltpu.make_async_remote_copy(
            src_ref=src, dst_ref=dst, send_sem=out, recv_sem=arrived,
            device_id=where, device_id_type=pl.DeviceIdType.MESH,
        )
        copy.start()
        sent.append(copy)

    def landed(ref, sem):
        pltpu.make_async_copy(ref, ref, sem).wait()

    sent = []
    load_raw = pltpu.make_async_copy(coef_in, raw, load_sem.at[0])
    load_raw.start()
    load_table = pltpu.make_async_copy(table_in, pair_table, load_sem.at[3])
    load_table.start()
    load_counts = pltpu.make_async_copy(counts_in, counts, load_sem.at[4])
    load_counts.start()
    load_zeta = pltpu.make_async_copy(zeta_in, zeta, load_sem.at[1])
    load_zeta.start()
    load_orb = pltpu.make_async_copy(orb_in, orb, load_sem.at[2])
    load_orb.start()
    barrier = pltpu.get_barrier_semaphore()
    greeted = [
        near(before, 0), near(before, 1), near(after, 0), near(after, 1), at_y[1], at_y[2], at_y[3], at_z, at_c,
        relay_to, relay_from, forward_to, forward_from,
    ]
    for where in greeted:
        pl.semaphore_signal(barrier, inc=1, device_id=where, device_id_type=pl.DeviceIdType.MESH)
    load_table.wait()
    load_counts.wait()
    load_raw.wait()
    for k in range(kpts):
        swap = jnp.full(raw.shape[2:], pair_table[0, k], jnp.int32) == 1
        one, two = raw[k, 0], raw[k, 1]
        picked[k] = jnp.where(swap, one, two)
        near_set = jnp.where(swap, two, one)
        picked[kpts + k] = near_set
        coef[kpts + k, z, y, c] = near_set
    pl.semaphore_wait(barrier, len(greeted))

    wide, narrow = pl.ds(0, bands), bands // 2
    halves = (pl.ds(0, narrow), pl.ds(narrow, narrow))
    last = kpts - 1
    pieces = [(0, cols) for cols in halves] + [(k, wide) for k in range(1, last)] + [(last, cols) for cols in halves]
    units = [(k, wide) for k in range(last)] + [(last, cols) for cols in halves]
    for n, (k, cols) in enumerate(pieces):
        for zz in range(NZ):
            send(picked.at[k, :, cols], coef.at[k, z, y, c, :, cols], pair_out.at[n, zz], pair_sem.at[n, z], near(before, zz))
    nearest, pack = pl.ds(kpts, kpts), kpts // 2
    send(picked.at[nearest], coef.at[nearest, z, y, c], cz_sem.at[1], cz_sem.at[0], at_z)

    def view(n, at, cc):
        if n >= len(pieces):
            return coef.at[pl.ds(kpts + (n - len(pieces)) * pack, pack), :, at, cc]
        return coef.at[pieces[n][0], :, at, cc, :, pieces[n][1]]

    def spread(n):
        for lane, where in enumerate((at_y[1], at_y[3], at_y[2], at_c)):
            send(view(n, y, c), view(n, y, c), ag_out.at[n, lane], ag_sem.at[n, lane], where)

    def pass_on(n):
        for lane, at in enumerate((ys[3], ys[1], ys[2])):
            landed(view(n, at, c), ag_sem.at[n, lane])
            send(view(n, at, c), view(n, at, c), ag_out.at[n, 4 + lane], ag_sem.at[n, 4 + lane], at_c)

    def joined(n):
        for lane, at in ((3, y), (4, ys[3]), (5, ys[1]), (6, ys[2])):
            landed(view(n, at, 1 - c), ag_sem.at[n, lane])

    def moved(n):
        k, cols = pieces[n]
        for zz in range(NZ):
            landed(coef.at[k, zz, y, c, :, cols], pair_sem.at[n, zz])

    def begin(n):
        if n == len(pieces):
            landed(coef.at[nearest, 1 - z, y, c], cz_sem.at[0])
        elif n < len(pieces):
            moved(n)
        spread(n)

    def product(ch, r, cols):
        lines = zeta[pl.ds(pl.multiple_of(r * tile, tile), tile), :]
        block = coef[ch, :, :, :, :, cols]
        return jnp.dot(lines, block.reshape(zeta.shape[1], block.shape[-1]), preferred_element_type=jnp.float32)

    def extra(k):
        return rows * RELAY[k] // RELAY_UNIT

    def parts(k):
        return pl.ds(0, rows - extra(k)), pl.ds(rows - extra(k), extra(k))

    def term(n):
        k, cols = pieces[n]

        def step(r, carry):
            value = product(k, r, cols)
            top = jnp.maximum(jnp.max(jnp.abs(value), axis=0, keepdims=True), 1e-30)
            level = jnp.round(value * (LEVELS / top)).astype(jnp.int32)
            psend[k, pl.ds(pl.multiple_of(r * tile, tile), tile), cols] = level.astype(jnp.int16)
            ssend[k, r, :, cols] = top / LEVELS
            return carry

        direct, other = parts(k)
        if n == 0:
            for side in range(2):
                lax.fori_loop(side * tiles // 2, (side + 1) * tiles // 2, step, 0)
                some = pl.ds(side * rows // 2, rows // 2)
                send(psend.at[k, some, cols], precv.at[k, some, cols], p_out.at[n, 2 * side], p_sem.at[n, 2 * side], at_after)
        else:
            lax.fori_loop(0, tiles, step, 0)
            if extra(k):
                send(psend.at[k, other], middle.at[k, pl.ds(0, extra(k))], relay_out.at[k, 0], relay_sem.at[k, 0], relay_to)
            send(psend.at[k, direct, cols], precv.at[k, direct, cols], p_out.at[n, 0], p_sem.at[n, 0], at_after)
        send(ssend.at[k, :, :, cols], srecv.at[k, :, :, cols], p_out.at[n, 1], p_sem.at[n, 1], at_after)

    def forward(k):
        if extra(k):
            held = middle.at[k, pl.ds(0, extra(k))]
            landed(held, relay_sem.at[k, 0])
            send(held, precv.at[k, parts(k)[1]], relay_out.at[k, 1], relay_sem.at[k, 1], forward_to)

    def own_term(k):
        def step(r, carry):
            field[k, pl.ds(pl.multiple_of(r * tile, tile), tile), :] = product(kpts + k, r, wide)
            return carry

        lax.fori_loop(0, tiles, step, 0)

    def arrived(u):
        k, wanted = units[u]
        direct, other = parts(k)
        for n, (owner, cols) in enumerate(pieces):
            if owner != k or wanted not in (wide, cols):
                continue
            if n == 0:
                for side in range(2):
                    landed(precv.at[k, pl.ds(side * rows // 2, rows // 2), cols], p_sem.at[n, 2 * side])
            else:
                landed(precv.at[k, direct, cols], p_sem.at[n, 0])
            landed(srecv.at[k, :, :, cols], p_sem.at[n, 1])
        if extra(k):
            landed(precv.at[k, other], relay_sem.at[k, 1])

    def combine(u):
        k, cols = units[u]
        lane = lax.broadcasted_iota(jnp.int32, (1, bands), 1)
        weight = jnp.where(lane[:, : cols.size] + cols.start < counts[k], 1.0, 0.0)
        weight_low = jnp.where(lane < counts[k], 1.0, 0.0).astype(jnp.bfloat16)

        def step(r, carry):
            at = pl.ds(pl.multiple_of(r * tile, tile), tile)
            level = precv[k, at, cols].astype(jnp.int32).astype(jnp.float32)
            value = (field[k, at, cols] + level * srecv[k, r, :, cols]) * weight
            field[k, at, cols] = value
            high = value.astype(jnp.bfloat16)
            low = (value - high.astype(jnp.float32)).astype(jnp.bfloat16)
            lines = orb[k, at, :] * weight_low
            over = (((0,), (0,)), ((), ()))
            added = lax.dot_general(lines, high, over, preferred_element_type=jnp.float32)
            added += lax.dot_general(lines, low, over, preferred_element_type=jnp.float32)
            added = added.reshape(*part.shape[1:4], cols.size)

            @pl.when(r == 0)
            def _():
                part[k, :, :, :, cols] = added

            @pl.when(r > 0)
            def _():
                part[k, :, :, :, cols] += added

            return carry

        lax.fori_loop(0, tiles, step, 0)
        send(part.at[k, 1 - c, :, :, cols], rsib.at[k, :, :, cols], ar_out.at[u, 0], ar_sem.at[u, 0], at_c)

    def scatter_y(u):
        k, cols = units[u]
        landed(rsib.at[k, :, :, cols], ar_sem.at[u, 0])
        half[k, :, :, cols] = part[k, c, :, :, cols] + rsib[k, :, :, cols]
        for d in range(1, NY):
            send(half.at[k, ys[d], :, cols], ry.at[k, d - 1, :, cols], ar_out.at[u, d], ar_sem.at[u, d], at_y[d])

    def swap_z(u):
        k, cols = units[u]
        total = half[k, y, :, cols]
        for d in range(1, NY):
            landed(ry.at[k, d - 1, :, cols], ar_sem.at[u, d])
            total = total + ry[k, d - 1, :, cols]
        quarter[k, :, cols] = total
        send(quarter.at[k, :, cols], rz.at[k, :, cols], ar_out.at[u, 4], ar_sem.at[u, 4], at_z)

    def gather_y(u):
        k, cols = units[u]
        landed(rz.at[k, :, cols], ar_sem.at[u, 4])
        final[k, c, y, :, cols] = quarter[k, :, cols] + rz[k, :, cols]
        done = final.at[k, c, y, :, cols]
        for d in range(1, NY):
            send(done, done, ar_out.at[u, 4 + d], ar_sem.at[u, 4 + d], at_y[d])

    def gather_c(u):
        k, cols = units[u]
        for d in range(1, NY):
            landed(final.at[k, c, ys[NY - d], :, cols], ar_sem.at[u, 4 + d])
        done = final.at[k, c, :, :, cols]
        send(done, done, ar_out.at[u, 8], ar_sem.at[u, 8], at_c)

    def settle(u):
        k, cols = units[u]
        landed(final.at[k, 1 - c, :, :, cols], ar_sem.at[u, 8])

    begin(0)
    load_zeta.wait()
    for n in range(len(pieces)):
        pass_on(n)
        begin(n + 1)
        joined(n)
        term(n)
    begin(7)
    forward(1)
    pass_on(6)
    forward(2)
    joined(6)
    own_term(0)
    own_term(1)
    load_orb.wait()
    arrived(0)
    combine(0)
    pass_on(7)
    scatter_y(0)
    joined(7)
    own_term(2)
    arrived(1)
    combine(1)
    swap_z(0)
    own_term(3)
    scatter_y(1)
    arrived(2)
    combine(2)
    swap_z(1)
    scatter_y(2)
    arrived(3)
    combine(3)
    swap_z(2)
    scatter_y(3)
    arrived(4)
    combine(4)
    swap_z(3)
    scatter_y(4)
    for u in range(4):
        gather_y(u)
    swap_z(4)
    gather_y(4)
    for u in range(5):
        gather_c(u)
    for u in range(5):
        settle(u)
    for copy in sent:
        copy.wait_send()


def exchange(zeta, coefs, orbitals, pair_table, counts):
    rows, points = zeta.shape
    kpts, _, share, bands = coefs.shape
    tile = min(TILE, rows)
    slice_ = bands // (NC * NY)
    f32, bf16, i16 = jnp.float32, jnp.bfloat16, jnp.int16
    hbm = pl.BlockSpec(memory_space=pltpu.HBM)
    vmem = pl.BlockSpec(memory_space=pltpu.VMEM)
    dma = pltpu.SemaphoreType.DMA
    most = rows * max(max(RELAY), 1) // RELAY_UNIT
    shapes = ((kpts, rows, bands), (kpts, NC, NY, slice_, bands))
    return pl.pallas_call(
        kernel,
        out_shape=tuple(pltpu.VMEM(shape, f32) for shape in shapes),
        in_specs=[hbm, hbm, hbm, hbm, hbm],
        out_specs=(vmem, vmem),
        scratch_shapes=[
            pltpu.SMEM((2, kpts), jnp.int32),
            pltpu.SMEM((kpts,), jnp.int32),
            pltpu.VMEM((rows, points), bf16),
            pltpu.VMEM((kpts, 2, share, bands), bf16),
            pltpu.VMEM((2 * kpts, share, bands), bf16),
            pltpu.VMEM((2 * kpts, NZ, NY, NC, share, bands), bf16),
            pltpu.VMEM((kpts, rows, bands), bf16),
            pltpu.VMEM((kpts, rows, bands), i16),
            pltpu.VMEM((kpts, rows, bands), i16),
            pltpu.VMEM((kpts, most, bands), i16),
            pltpu.VMEM((kpts, rows // tile, 1, bands), f32),
            pltpu.VMEM((kpts, rows // tile, 1, bands), f32),
            pltpu.VMEM((kpts, NC, NY, slice_, bands), f32),
            pltpu.VMEM((kpts, NY, slice_, bands), f32),
            pltpu.VMEM((kpts, NY, slice_, bands), f32),
            pltpu.VMEM((kpts, NY - 1, slice_, bands), f32),
            pltpu.VMEM((kpts, slice_, bands), f32),
            pltpu.VMEM((kpts, slice_, bands), f32),
            dma((5,)),
            dma((kpts + 2, NZ)),
            dma((kpts + 2, NZ)),
            dma((2,)),
            dma((kpts + 4, 7)),
            dma((kpts + 4, 7)),
            dma((kpts + 2, 3)),
            dma((kpts + 2, 3)),
            dma((kpts, 2)),
            dma((kpts, 2)),
            dma((kpts + 1, 9)),
            dma((kpts + 1, 9)),
        ],
        compiler_params=pltpu.CompilerParams(collective_id=0, has_side_effects=True, vmem_limit_bytes=61_800_000),
        name="exchange",
    )(pair_table.T, counts, zeta, coefs, orbitals)


def on_device(zeta_sets, coef_blocks, pair_table, band_counts, orbitals):
    fields, intersection = exchange(zeta_sets[0], coef_blocks, orbitals, pair_table, band_counts)
    kpts, bands = fields.shape[0], fields.shape[2]
    return fields, intersection.reshape(kpts, bands, bands)


def solution(mesh):
    return jax.shard_map(
        on_device,
        mesh=mesh,
        in_specs=(
            P("blk", "slab", None),
            P("blk", None, "slab", None),
            P("blk", None),
            P("blk"),
            P("blk", "slab", None),
        ),
        out_specs=(P("blk", "slab", None), P("blk", None, None)),
        check_vma=False,
    )
```
